32 devices in a mesh: pole: 4 (over x, core), row: 4 (over z), col: 2 (over y).
Axes of the slice: x: 2, y: 2, z: 4, core: 2. Of those that a mesh axis runs over, the one named last changes fastest.
Arguments:
- anc_inverse: bfloat16 [4, 2, 4, 192, 768], P('pole', None, None, 'col', 'row'), may hold values from -6 to 6
- panel: bfloat16 [4, 2, 768, 1024], P('pole', None, ('row', 'col')), may hold values from -0.21875 to 0.21875
- pattern: int32 [8, 2], replicated, may hold values 0 or 1
- diag_inverse: bfloat16 [4, 2, 1024, 512], P('pole', None, 'col', 'row'), may hold values from -6 to 6
- pole_weights: float32 [4, 2], P('pole'), may hold values from -4 to 4
Outputs:
- inv_panel: float32 [4, 2, 768, 1024], P('pole', None, 'row', 'col')
- inv_diag: bfloat16 [4, 2, 1024, 512], P('pole', None, 'col', 'row')
- density: float32 [1024, 512], P('col', 'row')
The draws below stay inside these ranges and needn't reach their ends.
All inputs are finite; a program needn't handle non-finite values.
Results may differ from the reference program's by a relative error of at most 0.013.
Values may be sent and summed in bfloat16 or wider, within the bound.
No kernel may reach another device: no remote copies, remote signals or barrier semaphores. Data moves between devices by JAX's collectives and lax.ppermute only.
A program may use at most 128 MiB of HBM per device.

```python
import jax
import jax.numpy as jnp
from jax import lax

W = 512
ANC_DEV = 96
POLES = 4
NK = 2
KW = 1024
NFB = 8
NA = 768
NQ = 4


def plant(values, rng, smallest, high):
    place = [jax.random.randint(jax.random.fold_in(rng, axis), (), 0, length) for axis, length in enumerate(values.shape)]
    main_axis = values.shape.index(max(values.shape))
    next_to = place[:main_axis] + [(place[main_axis] + 1) % values.shape[main_axis]] + place[main_axis + 1:]
    return values.at[tuple(place)].set(smallest).at[tuple(next_to)].set(high)


def block_scale(key, dims, pieces, smallest, top_value):
    factor_of = 1.0
    for axis_at, blocks in pieces:
        steps = jax.random.uniform(jax.random.fold_in(jax.random.fold_in(key, 6), axis_at), (blocks,), jnp.float32, smallest / len(pieces), top_value / len(pieces))
        factor_of = factor_of * jnp.repeat(jnp.exp(steps), dims[axis_at] // blocks).reshape((-1,) + (1,) * (len(dims) - 1 - axis_at))
    return factor_of


def bell_draw(own_key, dims, spread, most, split=(), held_as=jnp.bfloat16):
    loudness = block_scale(own_key, dims, split, -0.22, 0.18) if split else 1.0
    values = jax.random.normal(own_key, dims, jnp.float32) * spread * loudness
    return jnp.minimum(jnp.maximum(values, -most), most).astype(held_as)


def setup_inputs(seed: int = 0) -> dict:
    splits = jax.random.split(jax.random.key(seed), 6)
    return {
        "anc_inverse": bell_draw(splits[0], (POLES, 2, NQ, NA // NQ, NA), 1.0, 6.0, ((0, 4), (3, 2), (4, 4))),
        "panel": bell_draw(splits[1], (POLES, 2, NA, KW), NA ** -0.5, 0.21875, ((0, 4), (2, 8))),
        "pattern": plant((jax.random.randint(splits[2], (NFB, NK), 0, 3) < 2).astype(jnp.int32), jax.random.fold_in(splits[2], 1), 0, 1),
        "diag_inverse": bell_draw(splits[3], (POLES, 2, KW, W), 1.0, 6.0, ((0, 4), (2, 2), (3, 4))),
        "pole_weights": bell_draw(splits[4], (POLES, 2), 1.0, 4.0, ((0, 4),), jnp.float32),
    }


def complex_product(left_re, left_im, right_re, right_im):
    exact = lax.Precision.HIGHEST
    left_re = left_re.astype(jnp.float32)
    left_im = left_im.astype(jnp.float32)
    right_re = right_re.astype(jnp.float32)
    right_im = right_im.astype(jnp.float32)
    real_part = jnp.dot(left_re.T, right_re, precision=exact) - jnp.dot(left_im.T, right_im, precision=exact)
    imag_part = jnp.dot(left_im.T, right_re, precision=exact) + jnp.dot(left_re.T, right_im, precision=exact)
    return real_part, imag_part


def reference(anc_inverse, panel, pattern, diag_inverse, pole_weights):
    exact = lax.Precision.HIGHEST
    keep_mask = jnp.repeat(jnp.repeat(pattern.astype(jnp.bfloat16), W, axis=1), ANC_DEV, axis=0)

    def contract(first, second):
        return jnp.einsum('jka,jkb->kab', first, second, precision=exact)

    def one_pole(inputs):
        ancestor, factor, diagonal = inputs
        transposed = ancestor.reshape(2, NA, NA)
        masked = factor * keep_mask[None]
        prod_re, prod_im = complex_product(transposed[0], transposed[1], masked[0], masked[1])
        result_panel = jnp.stack([-prod_re, -prod_im])
        rounded = lax.optimization_barrier(result_panel.astype(jnp.bfloat16)).astype(jnp.float32)
        factor_full = masked.astype(jnp.float32).reshape(2, NA, NK, W)
        panel_full = rounded.reshape(2, NA, NK, W)
        diag_re = contract(factor_full[0], panel_full[0]) - contract(factor_full[1], panel_full[1])
        diag_im = contract(factor_full[0], panel_full[1]) + contract(factor_full[1], panel_full[0])
        result_diag = diagonal.astype(jnp.float32) - jnp.stack([diag_re, diag_im]).reshape(2, KW, W)
        return result_panel, result_diag

    inv_panel, diag_full = lax.map(one_pole, (anc_inverse, panel, diag_inverse))
    density = jnp.einsum('p,pab->ab', pole_weights[:, 0], diag_full[:, 1], precision=exact)
    density = density + jnp.einsum('p,pab->ab', pole_weights[:, 1], diag_full[:, 0], precision=exact)
    return inv_panel, diag_full.astype(jnp.bfloat16), density
```

```python
import jax
import jax.numpy as jnp
from jax import lax
from jax.sharding import PartitionSpec as P


def shift(value, axis, count, step):
    return lax.ppermute(value, axis, [(i, (i + step) % count) for i in range(count)])


def gather_slots(piece, row, n_row):
    if n_row != 4:
        return [piece] + [shift(piece, "row", n_row, -o) for o in range(1, n_row)]
    up = lax.ppermute(piece, "row", [(i + 1, i) for i in range(3)])
    down = lax.ppermute(piece, "row", [(i, i + 1) for i in range(3)])
    far = lax.ppermute(piece, "row", [(0, 2), (2, 0), (1, 3), (3, 1)])
    last = lax.ppermute(far, "row", [(2, 3), (1, 0)])
    return [piece, jnp.where(row == 3, last, up), far, jnp.where(row == 0, last, down)]


def col_order(pieces, col):
    if len(pieces) == 2:
        return [jnp.where(col == 0, pieces[0], pieces[1]), jnp.where(col == 0, pieces[1], pieces[0])]
    stacked = jnp.stack(pieces[::-1] * 2)
    count = len(pieces)
    rolled = lax.dynamic_slice_in_dim(stacked, (count - 1 - col) % count, count, 0)
    return [rolled[i] for i in range(count)]


def body(anc_inverse, panel, pattern, diag_inverse, pole_weights):
    n_row = lax.axis_size("row")
    n_col = lax.axis_size("col")
    n_pole = lax.axis_size("pole")
    row = lax.axis_index("row")
    col = lax.axis_index("col")
    block_rows = panel.shape[2]
    width = panel.shape[3] // n_col
    share = width // n_row
    row_count = anc_inverse.shape[4]
    keep = lax.dynamic_slice_in_dim(pattern, row * n_col + col, 1, 0)[0].astype(jnp.bfloat16)

    def masked_block(which):
        block = lax.dynamic_slice_in_dim(panel[0], which * width, width, 2)
        return block * lax.dynamic_index_in_dim(keep, which, 0, False)

    pieces = [masked_block(col)]
    segments = [anc_inverse[0]]
    for s in range(1, n_col):
        pieces.append(shift(masked_block((col + s) % n_col), "col", n_col, s))
    for s in range(1, n_col):
        segments.append(shift(anc_inverse[0], "col", n_col, s))
    slots = [gather_slots(piece, row, n_row) for piece in pieces]
    parts = []
    for o in range(n_row):
        parts.extend(col_order([slots[s][o] for s in range(n_col)], col))
    right = jnp.concatenate([part.reshape(2, 1, block_rows, width) for part in parts], axis=1)
    right = right.reshape(2 * n_row * n_col * block_rows, width)
    ordered = jnp.stack(col_order(segments, col), axis=2)
    turned = lax.dynamic_slice_in_dim(jnp.concatenate([ordered, ordered], axis=1), row, n_row, 1)
    turned = turned.reshape(2, n_row * n_col * block_rows, row_count)
    left = jnp.concatenate(
        [jnp.concatenate([turned[0], turned[1]], 1), jnp.concatenate([-turned[1], turned[0]], 1)], 0
    )
    product = lax.dot_general(left, right, (((0,), (0,)), ((), ())), preferred_element_type=jnp.float32)
    result_panel = -product.reshape(2, row_count, width)
    rounded = result_panel.astype(jnp.bfloat16)

    halves = []
    for o in range(n_row):
        block = lax.dynamic_slice_in_dim(rounded, ((row - o) % n_row) * share, share, 2)
        halves.append(block if o == 0 else shift(block, "row", n_row, -o))
    half_re = jnp.concatenate([h[0] for h in halves], 0)
    half_im = jnp.concatenate([h[1] for h in halves], 0)
    half = jnp.concatenate([jnp.concatenate([half_re, half_im], 1), jnp.concatenate([-half_im, half_re], 1)], 0)
    terms = lax.dot_general(right, half, (((0,), (0,)), ((), ())), preferred_element_type=jnp.float32)
    diag = diag_inverse[0].astype(jnp.float32)
    full_re = diag[0] - terms[:, :share]
    full_im = diag[1] - terms[:, share:]
    weight = pole_weights[0]
    total = weight[0] * full_im + weight[1] * full_re
    step = 1
    while step < n_pole:
        sent = total.astype(jnp.bfloat16)
        total = total + lax.ppermute(sent, "pole", [(i, i ^ step) for i in range(n_pole)]).astype(jnp.float32)
        step *= 2
    inv_diag = jnp.stack([full_re, full_im]).astype(jnp.bfloat16)
    return result_panel[None], inv_diag[None], total


def solution(mesh):
    placed = (
        P("pole", None, None, "col", "row"),
        P("pole", None, ("row", "col"), None),
        P(),
        P("pole", None, "col", "row"),
        P("pole", None),
    )
    return jax.shard_map(
        body,
        mesh=mesh,
        in_specs=placed,
        out_specs=(P("pole", None, "row", "col"), P("pole", None, "col", "row"), P("col", "row")),
        check_vma=False,
    )
```

```python
import jax
import jax.numpy as jnp
from jax import lax
from jax.experimental import pallas as pl
from jax.experimental.pallas import tpu as pltpu
from jax.sharding import PartitionSpec as P


def shift(value, axis, count, step):
    return lax.ppermute(value, axis, [(i, (i + step) % count) for i in range(count)])


def named(value, axis, pairs):
    return lax.ppermute(value, axis, pairs)


VMEM = pl.BlockSpec(memory_space=pltpu.VMEM)
SMEM = pl.BlockSpec(memory_space=pltpu.SMEM)


def cut_columns(panel, pattern, n_col, width):
    def kernel(pattern_ref, panel_ref, *out_refs):
        col = lax.axis_index("col")
        row = lax.axis_index("row")
        for s in range(n_col):
            which = lax.rem(col + s, n_col)
            keep = pattern_ref[row * n_col + col, which].astype(jnp.float32)
            block = panel_ref[:, :, pl.ds(pl.multiple_of(which * width, 128), width)]
            out_refs[s][...] = (block.astype(jnp.float32) * keep).astype(jnp.bfloat16)

    shape = jax.ShapeDtypeStruct(panel.shape[:2] + (width,), jnp.bfloat16)
    return pl.pallas_call(
        kernel,
        in_specs=[SMEM, VMEM],
        out_specs=[VMEM] * n_col,
        out_shape=[shape] * n_col,
        name="cut_columns",
    )(pattern, panel)


def contract(left, right):
    return lax.dot_general(left, right, (((0,), (0,)), ((), ())), preferred_element_type=jnp.float32)


def add_products(segment_ref, q, piece_ref, sums):
    real = segment_ref[0, q]
    imag = segment_ref[1, q]
    block = piece_ref[...]
    block = block.reshape(block.shape[0] * block.shape[1], block.shape[2])
    sum_re = contract(jnp.concatenate([real, -imag], 0), block)
    sum_im = contract(jnp.concatenate([imag, real], 0), block)
    return [sum_re, sum_im] if sums is None else [sums[0] + sum_re, sums[1] + sum_im]


def early_sum(segments, pieces, n_row):
    n_col = len(segments)

    def kernel(*refs):
        row = lax.axis_index("row")
        out_ref = refs[-1]
        sums = None
        for s in range(n_col):
            for o in range(n_row):
                q = lax.rem(row + o, n_row)
                sums = add_products(refs[s], q, refs[n_col + s * n_row + o], sums)
        out_ref[0] = sums[0]
        out_ref[1] = sums[1]

    operands = list(segments) + [piece for group in pieces for piece in group]
    shape = (2, segments[0].shape[3], pieces[0][0].shape[2])
    return pl.pallas_call(
        kernel,
        in_specs=[VMEM] * len(operands),
        out_specs=VMEM,
        out_shape=jax.ShapeDtypeStruct(shape, jnp.float32),
        name="early_sum",
    )(*operands)


def late_sum(early, segments, late, n_row):
    n_late = len(late)
    rows, width = early.shape[1:]
    share = width // n_row

    def kernel(*refs):
        row = lax.axis_index("row")
        early_ref = refs[0]
        result_ref = refs[1 + n_late * 2]
        half_refs = refs[2 + n_late * 2:-1]
        rounded_ref = refs[-1]
        sums = [early_ref[0], early_ref[1]]
        q = jnp.where(row == 0, n_row - 1, 0)
        for s in range(n_late):
            sums = add_products(refs[1 + s], q, refs[1 + n_late + s], sums)
        for part in range(2):
            value = -sums[part]
            result_ref[part] = value
            rounded_ref[part] = value.astype(jnp.bfloat16)
        for o in range(n_row):
            start = pl.multiple_of(lax.rem(row + n_row - o, n_row) * share, 128)
            half_refs[o][...] = rounded_ref[:, :, pl.ds(start, share)]

    operands = [early] + (list(segments) + list(late) if late else [])
    half = jax.ShapeDtypeStruct((2, rows, share), jnp.bfloat16)
    return pl.pallas_call(
        kernel,
        in_specs=[VMEM] * len(operands),
        out_specs=[VMEM] * (1 + n_row),
        out_shape=[jax.ShapeDtypeStruct(early.shape, jnp.float32)] + [half] * n_row,
        scratch_shapes=[pltpu.VMEM(early.shape, jnp.bfloat16)],
        name="late_sum",
    )(*operands)


def diagonal(weights, diag, halves, pieces, late):
    n_row = len(halves)
    n_col = len(pieces)
    n_late = len(late)
    block_rows, width = pieces[0][0].shape[1:]
    share = halves[0].shape[2]

    def kernel(weight_ref, diag_ref, *refs):
        row = lax.axis_index("row")
        col = lax.axis_index("col")
        half_refs = refs[:n_row]
        piece_refs = refs[n_row:n_row + n_col * n_row]
        late_refs = refs[n_row + n_col * n_row:-2]
        inv_ref, sent_ref = refs[-2:]
        total = None
        for s in range(n_col):
            start = pl.multiple_of(lax.rem(col + n_col - s, n_col) * block_rows, 16)
            blocks = [ref[:, pl.ds(start, block_rows), :] for ref in half_refs]
            uses = [(blocks[o], piece_refs[s * n_row + o]) for o in range(n_row)]
            if n_late:
                uses.append((jnp.where(row == 0, blocks[n_row - 1], blocks[1]), late_refs[s]))
            for half, piece_ref in uses:
                piece = piece_ref[...].reshape(2 * block_rows, width)
                upper = jnp.concatenate([half[0], half[1]], 1)
                lower = jnp.concatenate([-half[1], half[0]], 1)
                term = contract(jnp.concatenate([upper, lower], 0), piece)
                total = term if total is None else total + term
        full_re = diag_ref[0].astype(jnp.float32) - total[:share].T
        full_im = diag_ref[1].astype(jnp.float32) - total[share:].T
        inv_ref[0] = full_re.astype(jnp.bfloat16)
        inv_ref[1] = full_im.astype(jnp.bfloat16)
        sent_ref[...] = (weight_ref[0, 0] * full_im + weight_ref[0, 1] * full_re).astype(jnp.bfloat16)

    operands = list(halves) + [piece for group in pieces for piece in group] + list(late)
    return pl.pallas_call(
        kernel,
        in_specs=[SMEM] + [VMEM] * (1 + len(operands)),
        out_specs=[VMEM, VMEM],
        out_shape=[
            jax.ShapeDtypeStruct(diag.shape, jnp.bfloat16),
            jax.ShapeDtypeStruct(diag.shape[1:], jnp.bfloat16),
        ],
        name="diagonal",
    )(weights, diag, *operands)


def body(anc_inverse, panel, pattern, diag_inverse, pole_weights):
    n_row = lax.axis_size("row")
    n_col = lax.axis_size("col")
    n_pole = lax.axis_size("pole")
    width = panel.shape[3] // n_col
    cut = cut_columns(panel[0], pattern, n_col, width)
    ring_col = lambda s: [(i, (i + s) % n_col) for i in range(n_col)]
    firsts = [cut[0]] + [named(cut[s], "col", ring_col(s)) for s in range(1, n_col)]
    segments = [anc_inverse[0]] + [named(anc_inverse[0], "col", ring_col(s)) for s in range(1, n_col)]
    pieces = []
    late = []
    for piece in firsts:
        if n_row == 4:
            far = named(piece, "row", [(0, 2), (2, 0), (1, 3), (3, 1)])
            up = named(piece, "row", [(i + 1, i) for i in range(3)])
            down = named(piece, "row", [(i, i + 1) for i in range(3)])
            late.append(named(far, "row", [(2, 3), (1, 0)]))
            pieces.append([piece, up, far, down])
        else:
            pieces.append([piece] + [shift(piece, "row", n_row, -o) for o in range(1, n_row)])
    early = early_sum(segments, pieces, n_row)
    result_panel, *blocks = late_sum(early, segments, late, n_row)
    halves = [blocks[0]]
    for o in range(1, n_row):
        halves.append(named(blocks[o], "row", [(i, (i - o) % n_row) for i in range(n_row)]))
    inv_diag, total = diagonal(pole_weights, diag_inverse[0], halves, pieces, late)
    step = 1
    while step < n_pole:
        sent = total.astype(jnp.bfloat16)
        other = lax.ppermute(sent, "pole", [(i, i ^ step) for i in range(n_pole)])
        total = sent.astype(jnp.float32) + other.astype(jnp.float32)
        step *= 2
    return result_panel[None], inv_diag[None], total


def solution(mesh):
    placed = (
        P("pole", None, None, "col", "row"),
        P("pole", None, ("row", "col"), None),
        P(),
        P("pole", None, "col", "row"),
        P("pole", None),
    )
    return jax.shard_map(
        body,
        mesh=mesh,
        in_specs=placed,
        out_specs=(P("pole", None, "row", "col"), P("pole", None, "col", "row"), P("col", "row")),
        check_vma=False,
    )
```

```python
import jax
import jax.numpy as jnp
from jax import lax
from jax.experimental import pallas as pl
from jax.experimental.pallas import tpu as pltpu
from jax.sharding import PartitionSpec as P


def shift(value, axis, count, step):
    return lax.ppermute(value, axis, [(i, (i + step) % count) for i in range(count)])


VMEM = pl.BlockSpec(memory_space=pltpu.VMEM)
SMEM = pl.BlockSpec(memory_space=pltpu.SMEM)


def in_vmem(operands, near):
    if not near:
        return list(operands)
    return [pltpu.with_memory_space_constraint(operand, pltpu.VMEM) for operand in operands]


def result_of(near, shape, dtype):
    return pltpu.VMEM(shape, dtype) if near else jax.ShapeDtypeStruct(shape, dtype)


def cut_columns(panel, n_col, width, near):
    def kernel(panel_ref, *out_refs):
        col = lax.axis_index("col")
        for s in range(n_col):
            which = lax.rem(col + s, n_col)
            out_refs[s][...] = panel_ref[:, :, pl.ds(pl.multiple_of(which * width, 128), width)]

    return pl.pallas_call(
        kernel,
        in_specs=[VMEM],
        out_specs=[VMEM] * n_col,
        out_shape=[result_of(near, panel.shape[:2] + (width,), jnp.bfloat16)] * n_col,
        name="cut_columns",
    )(panel)


def kept(block, pattern_ref, q, s, n_col):
    col = lax.axis_index("col")
    keep = pattern_ref[q * n_col + lax.rem(col + n_col - s, n_col), col]
    return (block.astype(jnp.float32) * keep.astype(jnp.float32)).astype(jnp.bfloat16)


def contract(left, right):
    return lax.dot_general(left, right, (((0,), (0,)), ((), ())), preferred_element_type=jnp.float32)


def add_products(pattern_ref, segment_ref, q, s, n_col, piece_ref, sums):
    real = kept(segment_ref[0, q], pattern_ref, q, s, n_col)
    imag = kept(segment_ref[1, q], pattern_ref, q, s, n_col)
    block = piece_ref[...]
    block = block.reshape(block.shape[0] * block.shape[1], block.shape[2])
    sum_re = contract(jnp.concatenate([real, -imag], 0), block)
    sum_im = contract(jnp.concatenate([imag, real], 0), block)
    return [sum_re, sum_im] if sums is None else [sums[0] + sum_re, sums[1] + sum_im]


def early_sum(pattern, segments, pieces, n_row, near):
    n_col = len(segments)

    def kernel(pattern_ref, *refs):
        row = lax.axis_index("row")
        out_ref = refs[-1]
        sums = None
        for s in range(n_col):
            for o in range(n_row):
                q = lax.rem(row + o, n_row)
                sums = add_products(pattern_ref, refs[s], q, s, n_col, refs[n_col + s * n_row + o], sums)
        out_ref[0] = sums[0]
        out_ref[1] = sums[1]

    operands = list(segments) + in_vmem([piece for group in pieces for piece in group], near)
    shape = (2, segments[0].shape[3], pieces[0][0].shape[2])
    return pl.pallas_call(
        kernel,
        in_specs=[SMEM] + [VMEM] * len(operands),
        out_specs=VMEM,
        out_shape=result_of(near, shape, jnp.float32),
        name="early_sum",
    )(pattern, *operands)


def late_sum(pattern, early, segments, late, n_row, whole, near):
    n_col = len(segments)
    n_late = len(late)
    rows, width = early.shape[1:]
    share = width // n_row

    def kernel(pattern_ref, early_ref, *refs):
        row = lax.axis_index("row")
        outs = refs[2 * n_late:]
        sums = [early_ref[0], early_ref[1]]
        q = jnp.where(row == 0, n_row - 1, 0)
        for s in range(n_late):
            sums = add_products(pattern_ref, refs[s], q, s, n_col, refs[n_late + s], sums)
        if whole:
            outs[0][0] = -sums[0]
            outs[0][1] = -sums[1]
            return
        rounded_ref = outs[-1]
        rounded_ref[0] = (-sums[0]).astype(jnp.bfloat16)
        rounded_ref[1] = (-sums[1]).astype(jnp.bfloat16)
        for o in range(n_row):
            start = pl.multiple_of(lax.rem(row + n_row - o, n_row) * share, 128)
            outs[o][...] = rounded_ref[:, :, pl.ds(start, share)]

    operands = in_vmem([early], near) + (list(segments) + in_vmem(late, near) if late else [])
    half = result_of(near, (2, rows, share), jnp.bfloat16)
    return pl.pallas_call(
        kernel,
        in_specs=[SMEM] + [VMEM] * len(operands),
        out_specs=[VMEM] * (1 if whole else n_row),
        out_shape=[jax.ShapeDtypeStruct(early.shape, jnp.float32)] if whole else [half] * n_row,
        scratch_shapes=[] if whole else [pltpu.VMEM(early.shape, jnp.bfloat16)],
        name="whole_sum" if whole else "late_sum",
    )(pattern, *operands)


def diagonal(weights, pattern, diag, halves, pieces, late, near):
    n_row = len(halves)
    n_col = len(pieces)
    n_late = len(late)
    block_rows, width = pieces[0][0].shape[1:]
    share = halves[0].shape[2]

    def kernel(weight_ref, pattern_ref, diag_ref, *refs):
        row = lax.axis_index("row")
        col = lax.axis_index("col")
        half_refs = refs[:n_row]
        piece_refs = refs[n_row:n_row + n_col * n_row]
        late_refs = refs[n_row + n_col * n_row:-2]
        inv_ref, sent_ref = refs[-2:]
        total = None
        for s in range(n_col):
            start = pl.multiple_of(lax.rem(col + n_col - s, n_col) * block_rows, 16)
            blocks = [ref[:, pl.ds(start, block_rows), :] for ref in half_refs]
            uses = [(blocks[o], lax.rem(row + o, n_row), piece_refs[s * n_row + o]) for o in range(n_row)]
            if n_late:
                other = jnp.where(row == 0, blocks[n_row - 1], blocks[1])
                uses.append((other, jnp.where(row == 0, n_row - 1, 0), late_refs[s]))
            for half, q, piece_ref in uses:
                half = kept(half, pattern_ref, q, s, n_col)
                piece = piece_ref[...].reshape(2 * block_rows, width)
                upper = jnp.concatenate([half[0], half[1]], 1)
                lower = jnp.concatenate([-half[1], half[0]], 1)
                term = contract(jnp.concatenate([upper, lower], 0), piece)
                total = term if total is None else total + term
        full_re = diag_ref[0].astype(jnp.float32) - total[:share].T
        full_im = diag_ref[1].astype(jnp.float32) - total[share:].T
        inv_ref[0] = full_re.astype(jnp.bfloat16)
        inv_ref[1] = full_im.astype(jnp.bfloat16)
        sent_ref[...] = (weight_ref[0, 0] * full_im + weight_ref[0, 1] * full_re).astype(jnp.bfloat16)

    operands = in_vmem(list(halves) + [piece for group in pieces for piece in group] + list(late), near)
    return pl.pallas_call(
        kernel,
        in_specs=[SMEM, SMEM] + [VMEM] * (1 + len(operands)),
        out_specs=[VMEM, VMEM],
        out_shape=[
            jax.ShapeDtypeStruct(diag.shape, jnp.bfloat16),
            result_of(near, diag.shape[1:], jnp.bfloat16),
        ],
        name="diagonal",
    )(weights, pattern, diag, *operands)


def body(anc_inverse, panel, pattern, diag_inverse, pole_weights):
    n_row = lax.axis_size("row")
    n_col = lax.axis_size("col")
    n_pole = lax.axis_size("pole")
    width = panel.shape[3] // n_col
    held = 2 * width * (2 * panel.shape[2] * n_col * (n_row + 1) + 4 * anc_inverse.shape[4])
    near = held <= 3 * 2**20
    cut = cut_columns(panel[0], n_col, width, near)
    ring_col = lambda s: [(i, (i + s) % n_col) for i in range(n_col)]
    firsts = [cut[0]] + [lax.ppermute(cut[s], "col", ring_col(s)) for s in range(1, n_col)]
    segments = [anc_inverse[0]] + [lax.ppermute(anc_inverse[0], "col", ring_col(s)) for s in range(1, n_col)]
    pieces = []
    late = []
    for piece in firsts:
        if n_row == 4:
            far = lax.ppermute(piece, "row", [(0, 2), (2, 0), (1, 3), (3, 1)])
            up = lax.ppermute(piece, "row", [(i + 1, i) for i in range(3)])
            down = lax.ppermute(piece, "row", [(i, i + 1) for i in range(3)])
            late.append(lax.ppermute(far, "row", [(2, 3), (1, 0)]))
            pieces.append([piece, up, far, down])
        else:
            pieces.append([piece] + [shift(piece, "row", n_row, -o) for o in range(1, n_row)])
    early = early_sum(pattern, segments, pieces, n_row, near)
    blocks = late_sum(pattern, early, segments, late, n_row, False, near)
    (result_panel,) = late_sum(pattern, early, segments, late, n_row, True, near)
    halves = [blocks[0]]
    for o in range(1, n_row):
        halves.append(lax.ppermute(blocks[o], "row", [(i, (i - o) % n_row) for i in range(n_row)]))
    inv_diag, total = diagonal(pole_weights, pattern, diag_inverse[0], halves, pieces, late, near)
    step = 1
    while step < n_pole:
        sent = total.astype(jnp.bfloat16)
        other = lax.ppermute(sent, "pole", [(i, i ^ step) for i in range(n_pole)])
        total = sent.astype(jnp.float32) + other.astype(jnp.float32)
        step *= 2
    return result_panel[None], inv_diag[None], total


def solution(mesh):
    placed = (
        P("pole", None, None, "col", "row"),
        P("pole", None, ("row", "col"), None),
        P(),
        P("pole", None, "col", "row"),
        P("pole", None),
    )
    return jax.shard_map(
        body,
        mesh=mesh,
        in_specs=placed,
        out_specs=(P("pole", None, "row", "col"), P("pole", None, "col", "row"), P("col", "row")),
        check_vma=False,
    )
```

```python
import jax
import jax.numpy as jnp
from jax import lax
from jax.experimental import pallas as pl
from jax.experimental.pallas import tpu as pltpu
from jax.sharding import PartitionSpec as P


def shift(value, axis, count, step):
    return lax.ppermute(value, axis, [(i, (i + step) % count) for i in range(count)])


def named(value, axis, pairs):
    return lax.ppermute(value, axis, pairs)


VMEM = pl.BlockSpec(memory_space=pltpu.VMEM)
SMEM = pl.BlockSpec(memory_space=pltpu.SMEM)


def in_vmem(operands, near):
    if not near:
        return list(operands)
    return [pltpu.with_memory_space_constraint(operand, pltpu.VMEM) for operand in operands]


def result_of(near, shape, dtype):
    return pltpu.VMEM(shape, dtype) if near else jax.ShapeDtypeStruct(shape, dtype)


def cut_columns(panel, n_col, width, near):
    def kernel(panel_ref, *out_refs):
        col = lax.axis_index("col")
        for s in range(n_col):
            which = lax.rem(col + s, n_col)
            out_refs[s][...] = panel_ref[:, :, pl.ds(pl.multiple_of(which * width, 128), width)]

    return pl.pallas_call(
        kernel,
        in_specs=[VMEM],
        out_specs=[VMEM] * n_col,
        out_shape=[result_of(near, panel.shape[:2] + (width,), jnp.bfloat16)] * n_col,
        name="cut_columns",
    )(panel)


def kept(block, pattern_ref, q, s, n_col):
    col = lax.axis_index("col")
    keep = pattern_ref[q * n_col + lax.rem(col + n_col - s, n_col), col]
    return (block.astype(jnp.float32) * keep.astype(jnp.float32)).astype(jnp.bfloat16)


def source_row(row, o, n_row):
    return row ^ o if n_row == 4 else lax.rem(row + o, n_row)


def contract(left, right):
    return lax.dot_general(left, right, (((0,), (0,)), ((), ())), preferred_element_type=jnp.float32)


def add_products(pattern_ref, segment_ref, q, s, n_col, piece_ref, sums):
    real = kept(segment_ref[0, q], pattern_ref, q, s, n_col)
    imag = kept(segment_ref[1, q], pattern_ref, q, s, n_col)
    block = piece_ref[...]
    block = block.reshape(block.shape[0] * block.shape[1], block.shape[2])
    sum_re = contract(jnp.concatenate([real, -imag], 0), block)
    sum_im = contract(jnp.concatenate([imag, real], 0), block)
    return [sum_re, sum_im] if sums is None else [sums[0] + sum_re, sums[1] + sum_im]


def early_sum(pattern, segments, pieces, n_row, near):
    n_col = len(segments)

    def kernel(pattern_ref, *refs):
        row = lax.axis_index("row")
        out_ref = refs[-1]
        sums = None
        for s in range(n_col):
            for o in range(n_row):
                q = source_row(row, o, n_row)
                sums = add_products(pattern_ref, refs[s], q, s, n_col, refs[n_col + s * n_row + o], sums)
        out_ref[0] = sums[0]
        out_ref[1] = sums[1]

    operands = list(segments) + in_vmem([piece for group in pieces for piece in group], near)
    shape = (2, segments[0].shape[3], pieces[0][0].shape[2])
    return pl.pallas_call(
        kernel,
        in_specs=[SMEM] + [VMEM] * len(operands),
        out_specs=VMEM,
        out_shape=result_of(near, shape, jnp.float32),
        name="early_sum",
    )(pattern, *operands)


def late_sum(pattern, early, segments, late, n_row, whole, near):
    n_col = len(segments)
    n_late = len(late)
    rows, width = early.shape[1:]
    share = width // n_row

    def kernel(pattern_ref, early_ref, *refs):
        row = lax.axis_index("row")
        outs = refs[2 * n_late:]
        sums = [early_ref[0], early_ref[1]]
        q = source_row(row, n_row - 1, n_row)
        for s in range(n_late):
            sums = add_products(pattern_ref, refs[s], q, s, n_col, refs[n_late + s], sums)
        if whole:
            outs[0][0] = -sums[0]
            outs[0][1] = -sums[1]
            return
        rounded_ref = outs[-1]
        rounded_ref[0] = (-sums[0]).astype(jnp.bfloat16)
        rounded_ref[1] = (-sums[1]).astype(jnp.bfloat16)
        for o in range(n_row):
            target = row ^ o if n_row == 4 else lax.rem(row + n_row - o, n_row)
            start = pl.multiple_of(target * share, 128)
            outs[o][...] = rounded_ref[:, :, pl.ds(start, share)]

    operands = in_vmem([early], near) + (list(segments) + in_vmem(late, near) if late else [])
    half = result_of(near, (2, rows, share), jnp.bfloat16)
    return pl.pallas_call(
        kernel,
        in_specs=[SMEM] + [VMEM] * len(operands),
        out_specs=[VMEM] * (1 if whole else n_row),
        out_shape=[jax.ShapeDtypeStruct(early.shape, jnp.float32)] if whole else [half] * n_row,
        scratch_shapes=[] if whole else [pltpu.VMEM(early.shape, jnp.bfloat16)],
        name="whole_sum" if whole else "late_sum",
    )(pattern, *operands)


def diagonal(weights, pattern, diag, halves, pieces, late, near):
    n_row = len(halves)
    n_col = len(pieces)
    n_late = len(late)
    block_rows, width = pieces[0][0].shape[1:]
    share = halves[0].shape[2]

    def kernel(weight_ref, pattern_ref, diag_ref, *refs):
        row = lax.axis_index("row")
        col = lax.axis_index("col")
        half_refs = refs[:n_row]
        piece_refs = refs[n_row:n_row + n_col * n_row]
        late_refs = refs[n_row + n_col * n_row:-2]
        inv_ref, sent_ref = refs[-2:]
        total = None
        for s in range(n_col):
            start = pl.multiple_of(lax.rem(col + n_col - s, n_col) * block_rows, 16)
            blocks = [ref[:, pl.ds(start, block_rows), :] for ref in half_refs]
            uses = [(blocks[o], source_row(row, o, n_row), piece_refs[s * n_row + o]) for o in range(n_row)]
            if n_late:
                uses.append((blocks[-1], source_row(row, n_row - 1, n_row), late_refs[s]))
            for half, q, piece_ref in uses:
                half = kept(half, pattern_ref, q, s, n_col)
                piece = piece_ref[...].reshape(2 * block_rows, width)
                upper = jnp.concatenate([half[0], half[1]], 1)
                lower = jnp.concatenate([-half[1], half[0]], 1)
                term = contract(jnp.concatenate([upper, lower], 0), piece)
                total = term if total is None else total + term
        full_re = diag_ref[0].astype(jnp.float32) - total[:share].T
        full_im = diag_ref[1].astype(jnp.float32) - total[share:].T
        inv_ref[0] = full_re.astype(jnp.bfloat16)
        inv_ref[1] = full_im.astype(jnp.bfloat16)
        sent_ref[...] = (weight_ref[0, 0] * full_im + weight_ref[0, 1] * full_re).astype(jnp.bfloat16)

    operands = in_vmem(list(halves) + [piece for group in pieces for piece in group] + list(late), near)
    return pl.pallas_call(
        kernel,
        in_specs=[SMEM, SMEM] + [VMEM] * (1 + len(operands)),
        out_specs=[VMEM, VMEM],
        out_shape=[
            jax.ShapeDtypeStruct(diag.shape, jnp.bfloat16),
            result_of(near, diag.shape[1:], jnp.bfloat16),
        ],
        name="diagonal",
    )(weights, pattern, diag, *operands)


def body(anc_inverse, panel, pattern, diag_inverse, pole_weights):
    n_row = lax.axis_size("row")
    n_col = lax.axis_size("col")
    n_pole = lax.axis_size("pole")
    width = panel.shape[3] // n_col
    held = 2 * width * (2 * panel.shape[2] * n_col * (n_row + 1) + 4 * anc_inverse.shape[4])
    near = held <= 3 * 2**20
    cut = cut_columns(panel[0], n_col, width, near)
    ring_col = lambda s: [(i, (i + s) % n_col) for i in range(n_col)]
    firsts = [cut[0]] + [named(cut[s], "col", ring_col(s)) for s in range(1, n_col)]
    segments = [anc_inverse[0]] + [named(anc_inverse[0], "col", ring_col(s)) for s in range(1, n_col)]
    pieces = []
    late = []
    for piece in firsts:
        if n_row == 4:
            far = named(piece, "row", [(0, 2), (2, 0), (1, 3), (3, 1)])
            side = named(piece, "row", [(0, 1), (1, 0), (2, 3), (3, 2)])
            middle = named(piece, "row", [(1, 2), (2, 1)])
            late.append(named(far, "row", [(2, 3), (1, 0)]))
            pieces.append([piece, side, far, middle])
        else:
            pieces.append([piece] + [shift(piece, "row", n_row, -o) for o in range(1, n_row)])
    early = early_sum(pattern, segments, pieces, n_row, near)
    blocks = late_sum(pattern, early, segments, late, n_row, False, near)
    (result_panel,) = late_sum(pattern, early, segments, late, n_row, True, near)
    halves = [blocks[0]]
    for o in range(1, n_row):
        halves.append(named(blocks[o], "row", [(i, i ^ o if n_row == 4 else (i - o) % n_row) for i in range(n_row)]))
    inv_diag, total = diagonal(pole_weights, pattern, diag_inverse[0], halves, pieces, late, near)
    step = 1
    while step < n_pole:
        sent = total.astype(jnp.bfloat16)
        other = lax.ppermute(sent, "pole", [(i, i ^ step) for i in range(n_pole)])
        total = sent.astype(jnp.float32) + other.astype(jnp.float32)
        step *= 2
    return result_panel[None], inv_diag[None], total


def solution(mesh):
    placed = (
        P("pole", None, None, "col", "row"),
        P("pole", None, ("row", "col"), None),
        P(),
        P("pole", None, "col", "row"),
        P("pole", None),
    )
    return jax.shard_map(
        body,
        mesh=mesh,
        in_specs=placed,
        out_specs=(P("pole", None, "row", "col"), P("pole", None, "col", "row"), P("col", "row")),
        check_vma=False,
    )
```
